32 devices in a mesh: dp: 1 (over z), ey: 4 (over y), ex: 8 (over x, core).
Axes of the slice: x: 4, y: 4, z: 1, core: 2. Of those that a mesh axis runs over, the one named last changes fastest.
The devices are a block of a 4x4x8 slice.
Arguments:
- x: bfloat16 [16384, 2048], P(('dp', 'ey', 'ex'))
- ids: int32 [16384, 8], P(('dp', 'ey', 'ex'))
- gates: float32 [16384, 8], P(('dp', 'ey', 'ex'))
- w1: bfloat16 [64, 2048, 1024], P(('ey', 'ex'))
- w3: bfloat16 [64, 2048, 1024], P(('ey', 'ex'))
- w2: bfloat16 [64, 1024, 2048], P(('ey', 'ex'))
Outputs:
- output: bfloat16 [16384, 2048], P(('dp', 'ey', 'ex'))
All inputs are finite; a program needn't handle non-finite values.
Results may differ from the reference program's by a relative error of at most 0.00589437.
Values are sent between devices in bfloat16 or wider.
A program may use at most 768 MiB of HBM per device.

```python
import jax
import jax.numpy as jnp
from jax import lax

H = 2048
F = 1024
E = 64
TOP = 8
NG = 1
TG = 1
T = 512
P = 32

EL = E // P
N = P * T
GN = max(NG, 8)
GT = TG + (GN // 2 - TG) * (1 // NG)
EG = E // GN
CAP = min(T, 2 * T * TOP // P)


def setup_inputs(seed: int = 0, part: int = 0) -> dict:
    kw1, kw3, kw2 = jax.random.split(jax.random.key(seed), 3)
    kb1, kb2 = jax.random.split(jax.random.fold_in(jax.random.key(seed), 7), 2)
    kpart = jax.random.fold_in(jax.random.key(seed + 1), part)
    kx, _, _, ka = jax.random.split(kpart, 4)
    kg, ke = jax.random.split(jax.random.fold_in(kpart, 7), 2)
    x = jax.random.normal(kx, (N, H), jnp.float32)
    group_bias = jax.random.randint(kb1, (GN,), 0, 2 ** 21, jnp.int32)
    bias_draw = jax.random.randint(kb2, (E,), 0, 2 ** 10, jnp.int32)
    expert_bias = (3 * bias_draw * bias_draw) >> 1
    group_draw = jax.random.randint(kg, (N, GN), 0, 2 ** 20, jnp.int32)
    group_score = (group_draw + group_bias[None, :]) * GN + jnp.arange(GN, dtype=jnp.int32)[None, :]
    gtop = lax.top_k(group_score, GT)[1]
    gmask = jnp.any(gtop[:, :, None] == jnp.arange(GN)[None, None, :], axis=1)
    emask = jnp.repeat(gmask, EG, axis=1).astype(jnp.int32)
    expert_draw = jax.random.randint(ke, (N, E), 0, 2 ** 20, jnp.int32)
    expert_score = (expert_draw + expert_bias[None, :] + (4 << 20) * emask) * E + jnp.arange(E, dtype=jnp.int32)[None, :]
    ids = lax.top_k(expert_score, TOP)[1].astype(jnp.int32)
    a = jax.random.uniform(ka, (N, TOP), jnp.float32, 0.5, 1.5)
    gates = 2.5 * a / jnp.sum(a, axis=1, keepdims=True)
    w1 = jax.random.normal(kw1, (E, H, F), jnp.float32) * H ** -0.5
    w3 = jax.random.normal(kw3, (E, H, F), jnp.float32) * H ** -0.5
    w2 = jax.random.normal(kw2, (E, F, H), jnp.float32) * F ** -0.5
    return {"x": x.astype(jnp.bfloat16), "ids": ids, "gates": gates,
            "w1": w1.astype(jnp.bfloat16), "w3": w3.astype(jnp.bfloat16),
            "w2": w2.astype(jnp.bfloat16)}


def keep_mask(ids):
    dev = ids // EL
    hit = jnp.any(dev[:, :, None] == jnp.arange(P)[None, None, :], axis=1)
    hit3 = hit.reshape(P, T, P)
    rank = jnp.cumsum(hit3.astype(jnp.int32), axis=1) - 1
    kept = (hit3 & (rank < CAP)).reshape(N, P)
    return jnp.take_along_axis(kept, dev, axis=1)


def reference(x, ids, gates, w1, w3, w2):
    wk = gates * keep_mask(ids).astype(jnp.float32)

    def body(acc, e):
        c = jnp.sum(jnp.where(ids == e, wk, 0.0), axis=1)
        a1 = jnp.dot(x, w1[e], preferred_element_type=jnp.float32)
        a3 = jnp.dot(x, w3[e], preferred_element_type=jnp.float32)
        h = (jax.nn.silu(a1) * a3).astype(jnp.bfloat16)
        o = jnp.dot(h, w2[e], preferred_element_type=jnp.float32).astype(jnp.bfloat16)
        return acc + c[:, None] * o.astype(jnp.float32), None

    acc, _ = lax.scan(body, jnp.zeros((N, H), jnp.float32), jnp.arange(E))
    return (x.astype(jnp.float32) + acc).astype(jnp.bfloat16)
```

```python
import jax
import jax.numpy as jnp
from jax import lax
from jax.experimental import pallas as pl
from jax.experimental.pallas import tpu as pltpu
from jax.sharding import PartitionSpec as P

CAPF = 2
CHUNKS = 4
BLOCK = 512
TILE = 256


def expert_kernel(cnt, row_ref, col_ref, x_ref, w1_ref, w3_ref, w2_ref, o_ref):
    b = pl.program_id(0)
    el = w1_ref.shape[0]
    blk = x_ref.shape[0]
    o_ref[...] = jnp.zeros_like(o_ref)
    for e in range(el):
        n = cnt[b * el + e]

        def tile(i, carry):
            base = i * TILE
            rows = lax.broadcasted_iota(jnp.int32, (TILE, blk), 0) + base
            pick = jnp.where(row_ref[0, e:e + 1, :] == rows.astype(jnp.float32), 1.0, 0.0).astype(jnp.bfloat16)
            xs = jnp.dot(pick, x_ref[...], preferred_element_type=jnp.float32).astype(jnp.bfloat16)
            a1 = jnp.dot(xs, w1_ref[e], preferred_element_type=jnp.float32)
            a3 = jnp.dot(xs, w3_ref[e], preferred_element_type=jnp.float32)
            h = (jax.nn.silu(a1) * a3).astype(jnp.bfloat16)
            o = jnp.dot(h, w2_ref[e], preferred_element_type=jnp.float32).astype(jnp.bfloat16)
            cols = lax.broadcasted_iota(jnp.int32, (blk, TILE), 1) + base
            put = jnp.where(col_ref[0, :, e:e + 1] == cols.astype(jnp.float32), 1.0, 0.0).astype(jnp.bfloat16)
            s = jnp.dot(put, o, preferred_element_type=jnp.float32)
            o_ref[...] += col_ref[0, :, el + e:el + e + 1] * s
            return carry

        lax.fori_loop(0, (n + TILE - 1) // TILE, tile, 0)


def experts(cnt, rowp, colp, xg, w1, w3, w2):
    n, hd = xg.shape
    nb, el, blk = rowp.shape
    f = w1.shape[2]
    whole = lambda b, c: (0, 0, 0)
    once = pl.Buffered(1)
    return pl.pallas_call(
        expert_kernel,
        out_shape=jax.ShapeDtypeStruct((n, hd), jnp.float32),
        grid_spec=pltpu.PrefetchScalarGridSpec(
            num_scalar_prefetch=1,
            grid=(nb,),
            in_specs=[
                pl.BlockSpec((1, el, blk), lambda b, c: (b, 0, 0)),
                pl.BlockSpec((1, blk, colp.shape[2]), lambda b, c: (b, 0, 0)),
                pl.BlockSpec((blk, hd), lambda b, c: (b, 0)),
                pl.BlockSpec(w1.shape, whole, pipeline_mode=once),
                pl.BlockSpec(w3.shape, whole, pipeline_mode=once),
                pl.BlockSpec(w2.shape, whole, pipeline_mode=once),
            ],
            out_specs=pl.BlockSpec((blk, hd), lambda b, c: (b, 0)),
        ),
        compiler_params=pltpu.CompilerParams(vmem_limit_bytes=60 * 1024 * 1024),
        cost_estimate=pl.CostEstimate(
            flops=2 * 3 * n * hd * f, transcendentals=n * f, bytes_accessed=6 * n * hd + 6 * el * hd * f),
        name="experts",
    )(cnt, rowp, colp, xg, w1, w3, w2)


def solution(mesh):
    nx = mesh.shape["ex"]
    nd = mesh.shape["ey"] * nx
    axes = ("ey", "ex")
    tok = P(("dp", "ey", "ex"), None)
    wsp = P(("ey", "ex"), None, None)

    def local(x, ids, gates, w1, w3, w2):
        t, hd = x.shape
        top = ids.shape[1]
        el = w1.shape[0]
        cap = min(t, CAPF * t * top // nd)
        ct = t // CHUNKS
        xs = [lax.all_gather(x[c * ct:(c + 1) * ct], axes, axis=0, tiled=True) for c in range(CHUNKS)]

        eid = jnp.arange(nd * el)[:, None]
        coef = jnp.full((nd * el, t), -1.0, jnp.float32)
        for j in range(top):
            coef = jnp.where(ids[:, j][None, :] == eid, gates[:, j][None, :], coef)
        hit = jnp.any((coef >= 0).reshape(nd, el, t), axis=1)
        upto = (jnp.arange(t)[:, None] <= jnp.arange(t)[None, :]).astype(jnp.bfloat16)
        rank = jnp.dot(hit.astype(jnp.bfloat16), upto, preferred_element_type=jnp.float32)
        kept = hit & (rank <= cap)
        coef = jnp.where(kept[:, None, :], coef.reshape(nd, el, t), -1.0)
        mine = lax.all_to_all(coef, axes, 0, 0, tiled=True)

        spb = BLOCK // ct
        nb = nd // spb
        c4 = mine.reshape(nb, spb, el, CHUNKS, ct).transpose(3, 0, 2, 1, 4).reshape(CHUNKS, nb, el, BLOCK)
        sel = c4 >= 0
        within = (jnp.arange(BLOCK)[:, None] <= jnp.arange(BLOCK)[None, :]).astype(jnp.bfloat16)
        cum = jnp.dot(sel.reshape(-1, BLOCK).astype(jnp.bfloat16), within,
                      preferred_element_type=jnp.float32).reshape(sel.shape)
        place = jnp.where(sel, cum - 1.0, -1.0)
        counts = cum[..., -1].astype(jnp.int32).reshape(CHUNKS, nb * el)
        colp = jnp.concatenate([place, c4], axis=2).transpose(0, 1, 3, 2)

        outs = []
        for c in range(CHUNKS):
            part = experts(counts[c], place[c], colp[c], xs[c], w1, w3, w2)
            back = lax.psum_scatter(part, axes, scatter_dimension=0, tiled=True)
            outs.append((x[c * ct:(c + 1) * ct].astype(jnp.float32) + back).astype(jnp.bfloat16))
        return jnp.concatenate(outs, axis=0)

    return jax.shard_map(local, mesh=mesh, in_specs=(tok, tok, tok, wsp, wsp, wsp),
                         out_specs=tok, check_vma=False)
```

```python
import functools

import jax
import jax.numpy as jnp
import numpy as np
from jax import lax
from jax.experimental import pallas as pl
from jax.experimental.pallas import tpu as pltpu
from jax.sharding import Mesh, PartitionSpec as P

CAPF = 2
CORES = 2
CHUNKS = 4
BLOCK = 512
TILE = 256


def expert_kernel(nb, cnt, meta_ref, x_hbm, w1a, w3a, w2a, w1b, w3b, w2b, o_hbm,
                  xv, acc, b1, b3, b2, xsem, wsem, osem):
    e = pl.program_id(0)
    el = w1a.shape[0]
    ne = 2 * el
    slot = lax.rem(e, 2)

    def weights(k):
        a, i = ((w1a, w3a, w2a), k) if k < el else ((w1b, w3b, w2b), k - el)
        return [pltpu.make_async_copy(s.at[i], d.at[k % 2], wsem.at[k % 2, j])
                for j, (s, d) in enumerate(zip(a, (b1, b3, b2)))]

    def block(ref, b):
        return ref.at[pl.ds(pl.multiple_of(b * BLOCK, BLOCK), BLOCK), :]

    def load_x(b):
        return pltpu.make_async_copy(block(x_hbm, b), block(xv, b), xsem.at[b])

    def store_o(b):
        return pltpu.make_async_copy(block(acc, b), block(o_hbm, b), osem.at[b])

    @pl.when(e == 0)
    def _():
        load_x(0).start()
        for c in weights(0):
            c.start()
        for b in range(1, nb):
            load_x(b).start()

    for k in range(1, ne):
        @pl.when(e == k - 1)
        def _():
            for c in weights(k):
                c.start()

    for j, (s, d) in enumerate(((w1a, b1), (w3a, b3), (w2a, b2))):
        pltpu.make_async_copy(s.at[0], d.at[slot], wsem.at[slot, j]).wait()

    def one_block(b, carry):
        xb, ab = block(xv, b), block(acc, b)

        @pl.when(e == 0)
        def _():
            load_x(b).wait()
            ab[...] = jnp.zeros(ab.shape, ab.dtype)

        meta = meta_ref[b, e]
        col = meta.T

        def tile(i, carry):
            base = i * TILE
            rows = (lax.broadcasted_iota(jnp.int32, (TILE, BLOCK), 0) + base).astype(jnp.float32)
            pick = jnp.where(meta[0:1, :] == rows, 1.0, 0.0).astype(jnp.bfloat16)
            xs = jnp.dot(pick, xb[...], preferred_element_type=jnp.float32).astype(jnp.bfloat16)
            a1 = jnp.dot(xs, b1[slot], preferred_element_type=jnp.float32)
            a3 = jnp.dot(xs, b3[slot], preferred_element_type=jnp.float32)
            h = (jax.nn.silu(a1) * a3).astype(jnp.bfloat16)
            o = jnp.dot(h, b2[slot], preferred_element_type=jnp.float32).astype(jnp.bfloat16)
            cols = (lax.broadcasted_iota(jnp.int32, (BLOCK, TILE), 1) + base).astype(jnp.float32)
            put = jnp.where(col[:, 0:1] == cols, 1.0, 0.0).astype(jnp.bfloat16)
            ab[...] += col[:, 1:2] * jnp.dot(put, o, preferred_element_type=jnp.float32)
            return carry

        lax.fori_loop(0, (cnt[b * ne + e] + TILE - 1) // TILE, tile, 0)

        @pl.when(e == ne - 1)
        def _():
            store_o(b).start()

        return carry

    lax.fori_loop(0, nb, one_block, 0)

    @pl.when(e == ne - 1)
    def _():
        for b in range(nb):
            store_o(b).wait()


def experts(cnt, meta, xg, own, other):
    n, hd = xg.shape
    nb = n // BLOCK
    el, _, f = own[0].shape
    hbm = pl.BlockSpec(memory_space=pl.ANY)
    return pl.pallas_call(
        functools.partial(expert_kernel, nb),
        out_shape=jax.ShapeDtypeStruct((n, hd), jnp.float32),
        grid_spec=pltpu.PrefetchScalarGridSpec(
            num_scalar_prefetch=1,
            grid=(2 * el,),
            in_specs=[pl.BlockSpec(meta.shape, lambda e, c: (0, 0, 0, 0))] + [hbm] * 7,
            out_specs=hbm,
            scratch_shapes=[
                pltpu.VMEM((n, hd), jnp.bfloat16),
                pltpu.VMEM((n, hd), jnp.float32),
                pltpu.VMEM((2, hd, f), jnp.bfloat16),
                pltpu.VMEM((2, hd, f), jnp.bfloat16),
                pltpu.VMEM((2, f, hd), jnp.bfloat16),
                pltpu.SemaphoreType.DMA((nb,)),
                pltpu.SemaphoreType.DMA((2, 3)),
                pltpu.SemaphoreType.DMA((nb,)),
            ],
        ),
        compiler_params=pltpu.CompilerParams(vmem_limit_bytes=67043328, dimension_semantics=("arbitrary",)),
        cost_estimate=pl.CostEstimate(
            flops=2 * 3 * n * hd * f, transcendentals=n * f, bytes_accessed=6 * n * hd + 12 * el * hd * f),
        name="experts",
    )(cnt, meta, xg, *own, *other)


def solution(mesh):
    ny = mesh.shape["ey"]
    nx = mesh.shape["ex"] // CORES
    nd = ny * nx * CORES
    grid = Mesh(np.asarray(mesh.devices).reshape(mesh.shape["dp"], ny, nx, CORES), ("dp", "ey", "x", "core"))
    chips = ("ey", "x")
    tok = P(("dp", "ey", "x", "core"), None)
    wsp = P(("ey", "x", "core"), None, None)
    nc = ny * nx

    def local(x, ids, gates, w1, w3, w2):
        t, hd = x.shape
        top = ids.shape[1]
        el = w1.shape[0]
        ne = CORES * el
        cap = min(t, CAPF * t * top // nd)
        ct = t // CHUNKS
        xs = [lax.all_gather(x[c * ct:(c + 1) * ct], chips, axis=0, tiled=True) for c in range(CHUNKS)]
        swap = [(i, CORES - 1 - i) for i in range(CORES)]
        own = (w1, w3, w2)
        other = tuple(lax.ppermute(w, "core", swap) for w in own)

        eid = jnp.arange(nd * el)[:, None]
        coef = jnp.full((nd * el, t), -1.0, jnp.float32)
        for j in range(top):
            coef = jnp.where(ids[:, j][None, :] == eid, gates[:, j][None, :], coef)
        hit = jnp.any((coef >= 0).reshape(nd, el, t), axis=1)
        upto = (jnp.arange(t)[:, None] <= jnp.arange(t)[None, :]).astype(jnp.bfloat16)
        rank = jnp.dot(hit.astype(jnp.bfloat16), upto, preferred_element_type=jnp.float32)
        kept = hit & (rank <= cap)
        coef = jnp.where(kept[:, None, :], coef.reshape(nd, el, t), -1.0).reshape(nc, ne, t)
        mine = lax.all_to_all(coef, chips, 0, 0, tiled=True)
        mine = jnp.where(lax.axis_index("core") == 0, mine, jnp.roll(mine, el, axis=1))

        spb = BLOCK // ct
        nb = nc // spb
        c4 = mine.reshape(nb, spb, ne, CHUNKS, ct).transpose(3, 0, 2, 1, 4).reshape(CHUNKS * nb * ne, BLOCK)
        c4 = lax.optimization_barrier(c4)
        sel = c4 >= 0
        within = (jnp.arange(BLOCK)[:, None] <= jnp.arange(BLOCK)[None, :]).astype(jnp.bfloat16)
        cum = jnp.dot(sel.astype(jnp.bfloat16), within, preferred_element_type=jnp.float32)
        place = jnp.where(sel, cum - 1.0, -1.0)
        counts = cum[:, -1].astype(jnp.int32).reshape(CHUNKS, nb * ne)
        zero = jnp.zeros((6,) + place.shape, jnp.float32)
        meta = jnp.concatenate([place[None], c4[None], zero], axis=0).transpose(1, 0, 2)
        meta = meta.reshape(CHUNKS, nb, ne, 8, BLOCK)

        outs = []
        for c in range(CHUNKS):
            part = experts(counts[c], meta[c], xs[c], own, other)
            back = lax.psum_scatter(part, chips, scatter_dimension=0, tiled=True)
            outs.append((x[c * ct:(c + 1) * ct].astype(jnp.float32) + back).astype(jnp.bfloat16))
        return jnp.concatenate(outs, axis=0)

    return jax.shard_map(local, mesh=grid, in_specs=(tok, tok, tok, wsp, wsp, wsp),
                         out_specs=tok, check_vma=False)
```

```python
import jax
import jax.numpy as jnp
import numpy as np
from jax import lax
from jax.experimental import pallas as pl
from jax.experimental.pallas import tpu as pltpu
from jax.sharding import Mesh, PartitionSpec as P

CAPF = 2
CORES = 2
CHUNKS = 2
BLOCK = 512
SUB = 4
TILE = 256
HALF = 128


def expert_kernel(cnt, meta_ref, x_hbm, w1a, w3a, w2a, w1b, w3b, w2b, o_hbm,
                  xv, acc, b1, b3, b2, xsem, wsem, osem):
    g, e = pl.program_id(0), pl.program_id(1)
    ng = pl.num_programs(0)
    el = w1a.shape[0]
    ne = 2 * el
    slot = lax.rem(e, 2)
    last = e == ne - 1

    def weights(k):
        a, i = ((w1a, w3a, w2a), k) if k < el else ((w1b, w3b, w2b), k - el)
        return [pltpu.make_async_copy(s.at[i], d.at[k % 2], wsem.at[k % 2, j])
                for j, (s, d) in enumerate(zip(a, (b1, b3, b2)))]

    def block(ref, b):
        return ref.at[pl.ds(pl.multiple_of(b * BLOCK, BLOCK), BLOCK), :]

    def load_x(g, b):
        return pltpu.make_async_copy(block(x_hbm, g * SUB + b), block(xv, b), xsem.at[b])

    def store_o(g, b):
        return pltpu.make_async_copy(block(acc, b), block(o_hbm, g * SUB + b), osem.at[b])

    @pl.when((g == 0) & (e == 0))
    def _():
        load_x(0, 0).start()
        for c in weights(0):
            c.start()
        for b in range(1, SUB):
            load_x(0, b).start()

    @pl.when(last & (g < ng - 1))
    def _():
        for c in weights(0):
            c.start()

    for k in range(1, ne):
        @pl.when(e == k - 1)
        def _():
            for c in weights(k):
                c.start()

    for j, (s, d) in enumerate(((w1a, b1), (w3a, b3), (w2a, b2))):
        pltpu.make_async_copy(s.at[0], d.at[slot], wsem.at[slot, j]).wait()

    def one_block(b, carry):
        xb, ab = block(xv, b), block(acc, b)

        @pl.when((e == 0) & (g > 0))
        def _():
            store_o(g - 1, b).wait()

        @pl.when(e == 0)
        def _():
            load_x(g, b).wait()
            ab[...] = jnp.zeros(ab.shape, ab.dtype)

        meta = meta_ref[b, e]
        col = meta.T

        def tile(base, size):
            rows = (lax.broadcasted_iota(jnp.int32, (size, BLOCK), 0) + base).astype(jnp.float32)
            pick = jnp.where(meta[0:1, :] == rows, 1.0, 0.0).astype(jnp.bfloat16)
            xs = jnp.dot(pick, xb[...], preferred_element_type=jnp.float32).astype(jnp.bfloat16)
            a1 = jnp.dot(xs, b1[slot], preferred_element_type=jnp.float32)
            a3 = jnp.dot(xs, b3[slot], preferred_element_type=jnp.float32)
            h = (jax.nn.silu(a1) * a3).astype(jnp.bfloat16)
            o = jnp.dot(h, b2[slot], preferred_element_type=jnp.float32).astype(jnp.bfloat16)
            cols = (lax.broadcasted_iota(jnp.int32, (BLOCK, size), 1) + base).astype(jnp.float32)
            put = jnp.where(col[:, 0:1] == cols, 1.0, 0.0).astype(jnp.bfloat16)
            ab[...] += col[:, 1:2] * jnp.dot(put, o, preferred_element_type=jnp.float32)

        n = cnt[(g * SUB + b) * ne + e]
        full = (n + TILE - HALF - 1) // TILE

        def full_tile(i, carry):
            tile(i * TILE, TILE)
            return carry

        lax.fori_loop(0, full, full_tile, 0)

        @pl.when(n > full * TILE)
        def _():
            tile(full * TILE, HALF)

        @pl.when(last)
        def _():
            store_o(g, b).start()

        @pl.when(last & (g < ng - 1))
        def _():
            load_x(g + 1, b).start()

        return carry

    lax.fori_loop(0, SUB, one_block, 0)

    @pl.when(last & (g == ng - 1))
    def _():
        for b in range(SUB):
            store_o(g, b).wait()


def experts(cnt, meta, xg, own, other):
    n, hd = xg.shape
    m = SUB * BLOCK
    el, _, f = own[0].shape
    hbm = pl.BlockSpec(memory_space=pl.ANY)
    return pl.pallas_call(
        expert_kernel,
        out_shape=jax.ShapeDtypeStruct((n, hd), jnp.float32),
        grid_spec=pltpu.PrefetchScalarGridSpec(
            num_scalar_prefetch=1,
            grid=(n // m, 2 * el),
            in_specs=[pl.BlockSpec((SUB,) + meta.shape[1:], lambda g, e, c: (g, 0, 0, 0))] + [hbm] * 7,
            out_specs=hbm,
            scratch_shapes=[
                pltpu.VMEM((m, hd), jnp.bfloat16),
                pltpu.VMEM((m, hd), jnp.float32),
                pltpu.VMEM((2, hd, f), jnp.bfloat16),
                pltpu.VMEM((2, hd, f), jnp.bfloat16),
                pltpu.VMEM((2, f, hd), jnp.bfloat16),
                pltpu.SemaphoreType.DMA((SUB,)),
                pltpu.SemaphoreType.DMA((2, 3)),
                pltpu.SemaphoreType.DMA((SUB,)),
            ],
        ),
        compiler_params=pltpu.CompilerParams(
            vmem_limit_bytes=67043328, dimension_semantics=("arbitrary", "arbitrary")),
        cost_estimate=pl.CostEstimate(
            flops=2 * 3 * n * hd * f, transcendentals=n * f, bytes_accessed=6 * n * hd + 12 * el * hd * f),
        name="experts",
    )(cnt, meta, xg, *own, *other)


def solution(mesh):
    ny = mesh.shape["ey"]
    nx = mesh.shape["ex"] // CORES
    nd = ny * nx * CORES
    grid = Mesh(np.asarray(mesh.devices).reshape(mesh.shape["dp"], ny, nx, CORES), ("dp", "ey", "x", "core"))
    chips = ("ey", "x")
    tok = P(("dp", "ey", "x", "core"), None)
    wsp = P(("ey", "x", "core"), None, None)
    nc = ny * nx

    def local(x, ids, gates, w1, w3, w2):
        t, hd = x.shape
        top = ids.shape[1]
        el = w1.shape[0]
        ne = CORES * el
        cap = min(t, CAPF * t * top // nd)
        ct = t // CHUNKS
        xs = [lax.all_gather(x[c * ct:(c + 1) * ct], chips, axis=0, tiled=True) for c in range(CHUNKS)]
        swap = [(i, CORES - 1 - i) for i in range(CORES)]
        own = (w1, w3, w2)
        other = tuple(lax.ppermute(w, "core", swap) for w in own)

        eid = jnp.arange(nd * el)[:, None]
        coef = jnp.full((nd * el, t), -1.0, jnp.float32)
        for j in range(top):
            coef = jnp.where(ids[:, j][None, :] == eid, gates[:, j][None, :], coef)
        hit = jnp.any((coef >= 0).reshape(nd, el, t), axis=1)
        upto = (jnp.arange(t)[:, None] <= jnp.arange(t)[None, :]).astype(jnp.bfloat16)
        rank = jnp.dot(hit.astype(jnp.bfloat16), upto, preferred_element_type=jnp.float32)
        kept = hit & (rank <= cap)
        coef = jnp.where(kept[:, None, :], coef.reshape(nd, el, t), -1.0).reshape(nc, ne, t)
        mine = lax.all_to_all(coef, chips, 0, 0, tiled=True)
        mine = jnp.where(lax.axis_index("core") == 0, mine, jnp.roll(mine, el, axis=1))

        spb = BLOCK // ct
        nb = nc // spb
        c4 = mine.reshape(nb, spb, ne, CHUNKS, ct).transpose(3, 0, 2, 1, 4).reshape(CHUNKS * nb * ne, BLOCK)
        c4 = lax.optimization_barrier(c4)
        sel = c4 >= 0
        within = (jnp.arange(BLOCK)[:, None] <= jnp.arange(BLOCK)[None, :]).astype(jnp.bfloat16)
        cum = jnp.dot(sel.astype(jnp.bfloat16), within, preferred_element_type=jnp.float32)
        place = jnp.where(sel, cum - 1.0, -1.0)
        counts = cum[:, -1].astype(jnp.int32).reshape(CHUNKS, nb * ne)
        zero = jnp.zeros((6,) + place.shape, jnp.float32)
        meta = jnp.concatenate([place[None], c4[None], zero], axis=0).transpose(1, 0, 2)
        meta = meta.reshape(CHUNKS, nb, ne, 8, BLOCK)

        outs = []
        for c in range(CHUNKS):
            part = experts(counts[c], meta[c], xs[c], own, other)
            back = lax.psum_scatter(part, chips, scatter_dimension=0, tiled=True)
            outs.append((x[c * ct:(c + 1) * ct].astype(jnp.float32) + back).astype(jnp.bfloat16))
        return jnp.concatenate(outs, axis=0)

    return jax.shard_map(local, mesh=grid, in_specs=(tok, tok, tok, wsp, wsp, wsp),
                         out_specs=tok, check_vma=False)
```

```python
import jax
import jax.numpy as jnp
import numpy as np
from jax import lax
from jax.experimental import pallas as pl
from jax.experimental.pallas import tpu as pltpu
from jax.sharding import Mesh, PartitionSpec as P

CAPF = 2
CORES = 2
BLOCK = 512
SUB = 2
TILE = 256
HALF = 128


def expert_kernel(cnt, meta_ref, x_hbm, w1a, w3a, w2a, w1b, w3b, w2b, o_hbm,
                  xv, acc, b1, b3, b2, xsem, wsem, osem):
    g, e = pl.program_id(0), pl.program_id(1)
    ng = pl.num_programs(0)
    el = w1a.shape[0]
    ne = 2 * el
    slot = lax.rem(e, 2)
    last = e == ne - 1

    def weights(k):
        a, i = ((w1a, w3a, w2a), k) if k < el else ((w1b, w3b, w2b), k - el)
        return [pltpu.make_async_copy(s.at[i], d.at[k % 2], wsem.at[k % 2, j])
                for j, (s, d) in enumerate(zip(a, (b1, b3, b2)))]

    def block(ref, b):
        return ref.at[pl.ds(pl.multiple_of(b * BLOCK, BLOCK), BLOCK), :]

    def load_x(g, b):
        return pltpu.make_async_copy(block(x_hbm, g * SUB + b), block(xv, b), xsem.at[b])

    def store_o(g, b):
        return pltpu.make_async_copy(block(acc, b), block(o_hbm, g * SUB + b), osem.at[b])

    @pl.when((g == 0) & (e == 0))
    def _():
        load_x(0, 0).start()
        for c in weights(0):
            c.start()
        for b in range(1, SUB):
            load_x(0, b).start()

    @pl.when(last & (g < ng - 1))
    def _():
        for c in weights(0):
            c.start()

    for k in range(1, ne):
        @pl.when(e == k - 1)
        def _():
            for c in weights(k):
                c.start()

    for j, (s, d) in enumerate(((w1a, b1), (w3a, b3), (w2a, b2))):
        pltpu.make_async_copy(s.at[0], d.at[slot], wsem.at[slot, j]).wait()

    def one_block(b, carry):
        xb, ab = block(xv, b), block(acc, b)

        @pl.when((e == 0) & (g > 0))
        def _():
            store_o(g - 1, b).wait()

        @pl.when(e == 0)
        def _():
            load_x(g, b).wait()
            ab[...] = jnp.zeros(ab.shape, ab.dtype)

        meta = meta_ref[b, e]
        col = meta.T

        def tile(base, size):
            rows = (lax.broadcasted_iota(jnp.int32, (size, BLOCK), 0) + base).astype(jnp.float32)
            pick = jnp.where(meta[0:1, :] == rows, 1.0, 0.0).astype(jnp.bfloat16)
            xs = jnp.dot(pick, xb[...], preferred_element_type=jnp.float32).astype(jnp.bfloat16)
            a1 = jnp.dot(xs, b1[slot], preferred_element_type=jnp.float32)
            a3 = jnp.dot(xs, b3[slot], preferred_element_type=jnp.float32)
            h = (jax.nn.silu(a1) * a3).astype(jnp.bfloat16)
            o = jnp.dot(h, b2[slot], preferred_element_type=jnp.float32).astype(jnp.bfloat16)
            cols = (lax.broadcasted_iota(jnp.int32, (BLOCK, size), 1) + base).astype(jnp.float32)
            put = jnp.where(col[:, 0:1] == cols, 1.0, 0.0).astype(jnp.bfloat16)
            ab[...] += col[:, 1:2] * jnp.dot(put, o, preferred_element_type=jnp.float32)

        n = cnt[(g * SUB + b) * ne + e]
        full = (n + TILE - HALF - 1) // TILE

        def full_tile(i, carry):
            tile(i * TILE, TILE)
            return carry

        lax.fori_loop(0, full, full_tile, 0)

        @pl.when(n > full * TILE)
        def _():
            tile(full * TILE, HALF)

        @pl.when(last)
        def _():
            store_o(g, b).start()

        @pl.when(last & (g < ng - 1))
        def _():
            load_x(g + 1, b).start()

        return carry

    lax.fori_loop(0, SUB, one_block, 0)

    @pl.when(last & (g == ng - 1))
    def _():
        for b in range(SUB):
            store_o(g, b).wait()


def experts(cnt, meta, xg, own, other):
    n, hd = xg.shape
    m = SUB * BLOCK
    el, _, f = own[0].shape
    hbm = pl.BlockSpec(memory_space=pl.ANY)
    return pl.pallas_call(
        expert_kernel,
        out_shape=jax.ShapeDtypeStruct((n, hd), jnp.float32),
        grid_spec=pltpu.PrefetchScalarGridSpec(
            num_scalar_prefetch=1,
            grid=(n // m, 2 * el),
            in_specs=[pl.BlockSpec((SUB,) + meta.shape[1:], lambda g, e, c: (g, 0, 0, 0))] + [hbm] * 7,
            out_specs=hbm,
            scratch_shapes=[
                pltpu.VMEM((m, hd), jnp.bfloat16),
                pltpu.VMEM((m, hd), jnp.float32),
                pltpu.VMEM((2, hd, f), jnp.bfloat16),
                pltpu.VMEM((2, hd, f), jnp.bfloat16),
                pltpu.VMEM((2, f, hd), jnp.bfloat16),
                pltpu.SemaphoreType.DMA((SUB,)),
                pltpu.SemaphoreType.DMA((2, 3)),
                pltpu.SemaphoreType.DMA((SUB,)),
            ],
        ),
        compiler_params=pltpu.CompilerParams(
            vmem_limit_bytes=67043328, dimension_semantics=("arbitrary", "arbitrary")),
        cost_estimate=pl.CostEstimate(
            flops=2 * 3 * n * hd * f, transcendentals=n * f, bytes_accessed=6 * n * hd + 12 * el * hd * f),
        name="experts",
    )(cnt, meta, xg, *own, *other)


def solution(mesh):
    ny = mesh.shape["ey"]
    nx = mesh.shape["ex"] // CORES
    nd = ny * nx * CORES
    grid = Mesh(np.asarray(mesh.devices).reshape(mesh.shape["dp"], ny, nx, CORES), ("dp", "ey", "x", "core"))
    chips = ("ey", "x")
    tok = P(("dp", "ey", "x", "core"), None)
    wsp = P(("ey", "x", "core"), None, None)
    nc = ny * nx

    def local(x, ids, gates, w1, w3, w2):
        t, hd = x.shape
        top = ids.shape[1]
        el = w1.shape[0]
        ne = CORES * el
        cap = min(t, CAPF * t * top // nd)
        cut = 5 * t // 8
        parts = ((0, cut), (cut, t))
        xs = [lax.all_gather(x[a:b], chips, axis=0, tiled=True) for a, b in parts]
        swap = [(i, CORES - 1 - i) for i in range(CORES)]
        own = (w1, w3, w2)
        other = tuple(lax.ppermute(w, "core", swap) for w in own)

        eid = jnp.arange(nd * el)[:, None]
        coef = jnp.full((nd * el, t), -1.0, jnp.float32)
        for j in range(top):
            coef = jnp.where(ids[:, j][None, :] == eid, gates[:, j][None, :], coef)
        hit = jnp.any((coef >= 0).reshape(nd, el, t), axis=1)
        upto = (jnp.arange(t)[:, None] <= jnp.arange(t)[None, :]).astype(jnp.bfloat16)
        rank = jnp.dot(hit.astype(jnp.bfloat16), upto, preferred_element_type=jnp.float32)
        kept = hit & (rank <= cap)
        coef = jnp.where(kept[:, None, :], coef.reshape(nd, el, t), -1.0).reshape(nc, ne, t)
        mine = lax.all_to_all(coef, chips, 0, 0, tiled=True)
        mine = jnp.where(lax.axis_index("core") == 0, mine, jnp.roll(mine, el, axis=1))

        c4 = jnp.concatenate([mine[:, :, a:b].transpose(1, 0, 2).reshape(ne, -1, BLOCK).transpose(1, 0, 2)
                              for a, b in parts], axis=0).reshape(-1, BLOCK)
        c4 = lax.optimization_barrier(c4)
        sel = c4 >= 0
        within = (jnp.arange(BLOCK)[:, None] <= jnp.arange(BLOCK)[None, :]).astype(jnp.bfloat16)
        cum = jnp.dot(sel.astype(jnp.bfloat16), within, preferred_element_type=jnp.float32)
        place = jnp.where(sel, cum - 1.0, -1.0)
        counts = cum[:, -1].astype(jnp.int32)
        zero = jnp.zeros((6,) + place.shape, jnp.float32)
        meta = jnp.concatenate([place[None], c4[None], zero], axis=0).transpose(1, 0, 2)
        meta = meta.reshape(-1, ne, 8, BLOCK)

        outs = []
        for c, (a, b) in enumerate(parts):
            i, j = a * nc // BLOCK, b * nc // BLOCK
            part = experts(counts[i * ne:j * ne], meta[i:j], xs[c], own, other)
            back = lax.psum_scatter(part, chips, scatter_dimension=0, tiled=True)
            outs.append((x[a:b].astype(jnp.float32) + back).astype(jnp.bfloat16))
        return jnp.concatenate(outs, axis=0)

    return jax.shard_map(local, mesh=grid, in_specs=(tok, tok, tok, wsp, wsp, wsp),
                         out_specs=tok, check_vma=False)
```
